32 devices in a mesh: seq: 32 (over z, y, x, core).
Axes of the slice: x: 2, y: 2, z: 4, core: 2. Of those that a mesh axis runs over, the one named last changes fastest.
Arguments:
- queries: bfloat16 [32768, 4096], P('seq'), may hold values from -6 to 6
- span_keys: bfloat16 [32768, 1024], P('seq'), may hold values from -6 to 6
- span_values: bfloat16 [32768, 1024], P('seq'), may hold values from -6 to 6
- past_keys: bfloat16 [2, 32, 512, 1024], P(None, 'seq'), may hold values from -6 to 6
- past_values: bfloat16 [2, 32, 512, 1024], P(None, 'seq'), may hold values from -6 to 6
- selected: int32 [64, 8, 4], P('seq'), may hold values from 0 to 63, as said below
Outputs:
- attended: bfloat16 [32768, 4096], P('seq')
The draws below stay inside these ranges and needn't reach their ends.
Inputs may be any that keep to these rules, and one draw needn't show every extreme that they name: `selected`: query blocks k * 2 to (k + 1) * 2 - 1 form group k. Among the 64 numbers of one group, at most 2 are equal modulo 32, and some residue is named exactly 2 times.
All inputs are finite; a program needn't handle non-finite values.
Results may differ from the reference program's by a relative error of at most 0.005.
Values may be sent and summed in bfloat16 or wider, within the bound.
A program may use at most 256 MiB of HBM per device.

```python
import jax
import jax.numpy as jnp
from jax import lax

QH = 32
KVH = 8
HD = 128
BLOCK = 512
TOPK = 4
QB_DEV = 2
PB_DEV = 2
QTOK = 32768
N_SEQ = 32


def draw_queries(key, part):
    rows = BLOCK * QB_DEV * N_SEQ
    base = jnp.clip(jax.random.normal(jax.random.fold_in(key, 1), (rows, QH * HD), jnp.float32), -6.0, 6.0)
    return base.astype(jnp.bfloat16)


def draw_past_keys(key, part):
    base = jnp.clip(jax.random.normal(jax.random.fold_in(key, 5), (PB_DEV, N_SEQ, BLOCK, KVH * HD), jnp.float32), -6.0, 6.0)
    return base.astype(jnp.bfloat16)


def draw_selected(key, part):
    needed = QB_DEV * KVH * TOPK
    copies = (needed + N_SEQ - 1) // N_SEQ
    pool = jnp.tile(jnp.arange(N_SEQ, dtype=jnp.int32), copies)
    order_keys = jax.random.split(jax.random.fold_in(key, 11), N_SEQ)
    orders = jax.vmap(lambda item: jax.random.permutation(item, pool))(order_keys)
    owners = orders[:, :needed].reshape(N_SEQ * QB_DEV, KVH, TOPK).astype(jnp.int32)
    popular = jax.random.randint(jax.random.fold_in(key, 12), (N_SEQ,), 0, PB_DEV)
    favour = jax.random.randint(jax.random.fold_in(key, 13), (N_SEQ * QB_DEV, KVH, TOPK), 0, 10) < 6
    others = jax.random.randint(jax.random.fold_in(key, 14), (N_SEQ * QB_DEV, KVH, TOPK), 0, PB_DEV)
    local = jnp.where(favour, popular[owners], others)
    return (local * N_SEQ + owners).astype(jnp.int32)


def block_levels(key, shape, pieces, low, largest):
    gain = 1.0
    for dim, blocks in pieces:
        steps = jax.random.uniform(jax.random.fold_in(jax.random.fold_in(key, 6), dim), (blocks,), jnp.float32, low / len(pieces), largest / len(pieces))
        gain = gain * jnp.repeat(jnp.exp(steps), shape[dim] // blocks).reshape((-1,) + (1,) * (len(shape) - 1 - dim))
    return gain


def normal_values(rng, shape, scale, reach, cuts=(), kind=jnp.bfloat16):
    array = jax.random.normal(rng, shape, jnp.float32) * scale
    if len(cuts) > 0:
        array = block_levels(rng, shape, cuts, -0.22, 0.18) * array
    return jnp.clip(array, min=-reach, max=reach).astype(kind)


def setup_inputs(seed: int = 0) -> dict:
    arg_keys = jax.random.split(jax.random.key(seed), 7)
    queries = draw_queries(jax.random.fold_in(arg_keys[6], 71), 0)
    span_keys = normal_values(arg_keys[1], (QTOK, KVH * HD), 1.0, 6.0, ((0, 32),))
    span_values = normal_values(arg_keys[2], (QTOK, KVH * HD), 1.0, 6.0, ((0, 32),))
    past_keys = draw_past_keys(jax.random.fold_in(arg_keys[6], 71), 0)
    past_values = normal_values(arg_keys[4], (PB_DEV, N_SEQ, BLOCK, KVH * HD), 1.0, 6.0, ((1, 32),))
    selected = draw_selected(jax.random.fold_in(arg_keys[6], 71), 0)
    return dict(queries=queries, span_keys=span_keys, span_values=span_values, past_keys=past_keys, past_values=past_values, selected=selected)


def reference(queries, span_keys, span_values, past_keys, past_values, selected):
    group = QH // KVH
    scale = HD ** -0.5
    blocks_all = QB_DEV * N_SEQ
    query_blocks = queries.reshape(blocks_all, BLOCK, KVH, group, HD)
    near_keys_all = span_keys.reshape(blocks_all, BLOCK, KVH, HD)
    near_values_all = span_values.reshape(blocks_all, BLOCK, KVH, HD)
    far_keys_all = past_keys.reshape(PB_DEV * N_SEQ, BLOCK, KVH, HD)
    far_values_all = past_values.reshape(PB_DEV * N_SEQ, BLOCK, KVH, HD)
    head_ids = jnp.arange(KVH, dtype=jnp.int32)[:, None]
    causal = jnp.arange(BLOCK)[None, :] <= jnp.arange(BLOCK)[:, None]

    def one_block(items):
        query_block, near_keys, near_values, chosen = items
        far_keys = far_keys_all[chosen, :, head_ids, :].reshape(KVH, TOPK * BLOCK, HD).astype(jnp.float32)
        far_values = far_values_all[chosen, :, head_ids, :].reshape(KVH, TOPK * BLOCK, HD).astype(jnp.float32)
        query_wide = query_block.astype(jnp.float32)
        far = jnp.einsum("ihgd,hkd->hgik", query_wide, far_keys) * scale
        near = jnp.einsum("ihgd,jhd->hgij", query_wide, near_keys.astype(jnp.float32)) * scale
        near = jnp.where(causal, near, -jnp.inf)
        top = jnp.maximum(jnp.max(far, axis=-1), jnp.max(near, axis=-1))[..., None]
        far_weight = jnp.exp(far - top)
        near_weight = jnp.exp(near - top)
        total = jnp.sum(far_weight, axis=-1, keepdims=True) + jnp.sum(near_weight, axis=-1, keepdims=True)
        far_probs = (far_weight / total).astype(jnp.bfloat16).astype(jnp.float32)
        near_probs = (near_weight / total).astype(jnp.bfloat16).astype(jnp.float32)
        result = jnp.einsum("hgik,hkd->ihgd", far_probs, far_values)
        result = result + jnp.einsum("hgij,jhd->ihgd", near_probs, near_values.astype(jnp.float32))
        return result.astype(jnp.bfloat16).reshape(BLOCK, QH * HD)

    attended = lax.map(one_block, (query_blocks, near_keys_all, near_values_all, selected))
    return attended.reshape(blocks_all * BLOCK, QH * HD)
```

```python
import functools
import math

import jax
import jax.numpy as jnp
from jax import lax
from jax.experimental import pallas as pl
from jax.experimental.pallas import tpu as pltpu
from jax.sharding import PartitionSpec as P


GROUPS = 8


def owner_ranks(owners):
    length = owners.shape[-1]
    later = lax.broadcasted_iota(jnp.int32, (length, length), 0)
    sooner = lax.broadcasted_iota(jnp.int32, (length, length), 1)
    same = owners[..., :, None] == owners[..., None, :]
    return jnp.sum(jnp.where(same & (sooner < later), 1, 0), axis=-1).astype(jnp.int32)


def gather_kernel(count, slots, heads, width, request_ref, keys_ref, values_ref, *rest):
    outs, sems = rest[:count], rest[count]
    copies = []
    for turn in range(count):
        for slot in range(slots):
            request = request_ref[turn * slots + slot]
            block, head = request // heads, lax.rem(request, heads)
            lanes = pl.ds(pl.multiple_of(head * width, width), width)
            for kind, ref in ((0, keys_ref), (1, values_ref)):
                copy = pltpu.make_async_copy(
                    ref.at[block, 0, :, lanes],
                    outs[turn].at[slot, kind],
                    sems.at[turn * slots * 2 + slot * 2 + kind],
                )
                copy.start()
                copies.append(copy)
    for copy in copies:
        copy.wait()


def gather_requests(request, past_keys, past_values, count, slots, heads):
    block, width = past_keys.shape[2], past_keys.shape[3] // heads
    piece = jax.ShapeDtypeStruct((slots, 2, block, width), past_keys.dtype)
    return pl.pallas_call(
        functools.partial(gather_kernel, count, slots, heads, width),
        out_shape=[piece] * count,
        in_specs=[
            pl.BlockSpec(memory_space=pltpu.SMEM),
            pl.BlockSpec(memory_space=pltpu.VMEM),
            pl.BlockSpec(memory_space=pltpu.VMEM),
        ],
        out_specs=[pl.BlockSpec(memory_space=pl.ANY)] * count,
        scratch_shapes=[pltpu.SemaphoreType.DMA((count * slots * 2,))],
    )(request, past_keys, past_values)


def partial_attention(query_ref, keys, values, out_ref, stat_ref, group, mask):
    block, width = keys.shape
    factor = width**-0.5 * math.log2(math.e)
    values_t = values.T
    for member in range(group):
        query = query_ref[:, member * width : (member + 1) * width]
        span = slice(member * block, (member + 1) * block)
        scores = lax.dot_general(
            keys, query, (((1,), (1,)), ((), ())), preferred_element_type=jnp.float32
        )
        if mask is not None:
            scores = jnp.where(mask, scores, -jnp.inf)
        top = jnp.max(scores, axis=0, keepdims=True) * factor
        weights = jnp.exp2(scores * factor - top)
        stat_ref[0, 0:1, span] = top
        stat_ref[0, 1:2, span] = jnp.sum(weights, axis=0, keepdims=True)
        out_ref[0, :, span] = jnp.dot(
            values_t, weights.astype(jnp.bfloat16), preferred_element_type=jnp.float32
        ).astype(jnp.bfloat16)


def near_kernel(group, query_ref, keys_ref, values_ref, out_ref, stat_ref):
    block = keys_ref.shape[0]
    mask = lax.broadcasted_iota(jnp.int32, (block, block), 0) <= lax.broadcasted_iota(
        jnp.int32, (block, block), 1
    )
    partial_attention(
        query_ref, keys_ref[...], values_ref[...], out_ref, stat_ref, group, mask
    )


def far_kernel(group, rows_ref, query_ref, pair_ref, _out, _stat, out_ref, stat_ref):
    partial_attention(
        query_ref, pair_ref[0, 0], pair_ref[0, 1], out_ref, stat_ref, group, None
    )


def merge_kernel(group, picks, places_ref, *refs):
    outs, stats, result_ref = refs[: picks + 1], refs[picks + 1 : 2 * picks + 2], refs[-1]
    width = outs[0].shape[1]
    block = result_ref.shape[0]
    for member in range(group):
        span = slice(member * block, (member + 1) * block)
        tops = [stat[0, 0:1, span] for stat in stats]
        top = functools.reduce(jnp.maximum, tops)
        scales = [jnp.exp2(item - top) for item in tops]
        total = sum(scale * stat[0, 1:2, span] for scale, stat in zip(scales, stats))
        inverse = 1.0 / total
        mixed = sum(
            out[0, :, span].astype(jnp.float32) * (scale * inverse)
            for out, scale in zip(outs, scales)
        )
        result_ref[:, member * width : (member + 1) * width] = mixed.T.astype(jnp.bfloat16)


def shards(queries, span_keys, span_values, past_keys, past_values, selected):
    count = lax.axis_size("seq")
    me = lax.axis_index("seq")
    local_blocks, heads, picks = selected.shape
    needed = local_blocks * heads * picks
    rows = local_blocks * heads
    slots = (needed + count - 1) // count
    block = queries.shape[0] // local_blocks
    width = past_keys.shape[-1] // heads
    group = queries.shape[1] // (heads * width)
    span = group * block

    chosen = selected.reshape(-1)
    owners = chosen % count
    ranks = owner_ranks(owners)
    head_flat = lax.broadcasted_iota(jnp.int32, selected.shape, 1).reshape(-1)
    wanted = chosen // count * heads + head_flat
    slot_ids = owners * slots + ranks
    match = slot_ids[None, :] == jnp.arange(count * slots, dtype=jnp.int32)[:, None]
    outgoing = jnp.sum(jnp.where(match, wanted[None, :], 0), axis=1).reshape(count, slots)
    incoming = lax.all_to_all(outgoing, "seq", split_axis=0, concat_axis=0, tiled=True)

    turns = [0]
    for step in range(1, count // 2 + 1):
        turns.append(step)
        if step != count - step:
            turns.append(count - step)
    turns_array = jnp.array(turns, dtype=jnp.int32)
    request = jnp.take(incoming, (me + turns_array) % count, axis=0).reshape(-1)
    sources = (me - turns_array) % count
    place_ids = (sources[:, None] * slots + jnp.arange(slots, dtype=jnp.int32)).reshape(-1)
    found = place_ids[:, None] == slot_ids[None, :]
    pick_rows = jnp.arange(needed, dtype=jnp.int32) // picks
    pair_rows = jnp.sum(jnp.where(found, pick_rows[None, :], 0), axis=1).astype(jnp.int32)
    place_of = jnp.sum(
        jnp.where(found, jnp.arange(count * slots, dtype=jnp.int32)[:, None], 0), axis=0
    ).astype(jnp.int32)

    pieces = gather_requests(request, past_keys, past_values, count, slots, heads)
    arrived = [pieces[0]]
    for turn, piece in zip(turns[1:], pieces[1:]):
        arrived.append(
            lax.ppermute(piece, "seq", [(d, (d + turn) % count) for d in range(count)])
        )

    places = count * slots + rows
    partial_shapes = [
        jax.ShapeDtypeStruct((places, width, span), jnp.bfloat16),
        jax.ShapeDtypeStruct((places, 2, span), jnp.float32),
    ]
    pair_cost = 4 * span * block * width
    outs, stats = pl.pallas_call(
        functools.partial(near_kernel, group),
        grid=(rows,),
        in_specs=[
            pl.BlockSpec((block, group * width), lambda i: (i // heads, i % heads)),
            pl.BlockSpec((block, width), lambda i: (i // heads, i % heads)),
            pl.BlockSpec((block, width), lambda i: (i // heads, i % heads)),
        ],
        out_specs=[
            pl.BlockSpec((1, width, span), lambda i: (i + count * slots, 0, 0)),
            pl.BlockSpec((1, 2, span), lambda i: (i + count * slots, 0, 0)),
        ],
        out_shape=partial_shapes,
        cost_estimate=pl.CostEstimate(
            flops=rows * pair_cost, bytes_accessed=rows * 1500000, transcendentals=0
        ),
    )(queries, span_keys, span_values)

    size = max(count // GROUPS, 1)
    for first in range(0, count, size):
        pairs = jnp.concatenate(arrived[first : first + size], axis=0)
        length = pairs.shape[0]
        base = first * slots
        outs, stats = pl.pallas_call(
            functools.partial(far_kernel, group),
            grid_spec=pltpu.PrefetchScalarGridSpec(
                num_scalar_prefetch=1,
                grid=(length,),
                in_specs=[
                    pl.BlockSpec(
                        (block, group * width),
                        lambda i, r: (r[i] // heads, lax.rem(r[i], heads)),
                    ),
                    pl.BlockSpec((1, 2, block, width), lambda i, r: (i, 0, 0, 0)),
                    pl.BlockSpec(memory_space=pl.ANY),
                    pl.BlockSpec(memory_space=pl.ANY),
                ],
                out_specs=[
                    pl.BlockSpec((1, width, span), lambda i, r, base=base: (i + base, 0, 0)),
                    pl.BlockSpec((1, 2, span), lambda i, r, base=base: (i + base, 0, 0)),
                ],
            ),
            out_shape=partial_shapes,
            input_output_aliases={3: 0, 4: 1},
            cost_estimate=pl.CostEstimate(
                flops=length * pair_cost, bytes_accessed=length * 1500000, transcendentals=0
            ),
        )(lax.dynamic_slice_in_dim(pair_rows, base, length), queries, pairs, outs, stats)

    def far_place(pick):
        return lambda i, p: (p[i * picks + pick], 0, 0)

    maps = [far_place(pick) for pick in range(picks)]
    maps.append(lambda i, p: (i + count * slots, 0, 0))
    return pl.pallas_call(
        functools.partial(merge_kernel, group, picks),
        grid_spec=pltpu.PrefetchScalarGridSpec(
            num_scalar_prefetch=1,
            grid=(rows,),
            in_specs=[pl.BlockSpec((1, width, span), item) for item in maps]
            + [pl.BlockSpec((1, 2, span), item) for item in maps],
            out_specs=pl.BlockSpec(
                (block, group * width), lambda i, p: (i // heads, i % heads)
            ),
        ),
        out_shape=jax.ShapeDtypeStruct(queries.shape, queries.dtype),
    )(place_of, *([outs] * (picks + 1)), *([stats] * (picks + 1)))


def solution(mesh):
    return jax.shard_map(
        shards,
        mesh=mesh,
        in_specs=(
            P("seq", None),
            P("seq", None),
            P("seq", None),
            P(None, "seq", None, None),
            P(None, "seq", None, None),
            P("seq", None, None),
        ),
        out_specs=P("seq", None),
        check_vma=False,
    )
```
